32 devices in a mesh: member: 2 (over core), tile: 16 (over z, y, x).
Axes of the slice: x: 2, y: 2, z: 4, core: 2. Of those that a mesh axis runs over, the one named last changes fastest.
Arguments:
- ensemble: bfloat16 [40, 7, 32, 2048], P('member', None, None, 'tile'), may hold values from -6 to 6
- control: bfloat16 [40, 32, 2048], P('member', None, 'tile'), may hold values from -6 to 6
- vert_loc: bfloat16 [32, 32], replicated, may hold values from -1 to 1
- obs_source: int32 [8192, 1], P('tile'), may hold values from 0 to 15; in each aligned block of 512 rows (0 to 511, 512 to 1023, ...) at most 64 rows name the same one
- obs_column: int32 [8192], P('tile'), may hold values from 0 to 127
- obs_slot: int32 [8192], P('tile'), may hold values from 0 to 5
- obs_frac: float32 [8192], P('tile'), may hold values from 0 to 1
- obs_count: int32 [16], P('tile'), may hold values from 1 to 512, 4096 in all
Outputs:
- obs_increment: float32 [32, 8192], P(None, 'tile')
The draws below stay inside these ranges and needn't reach their ends.
Inputs may be any that keep to these rules, and one draw needn't show every extreme that they name: `obs_source`: among the 512 observation slots of one owner tile, at most 64 name the same source tile, and some source tile is named exactly 64 times. `obs_count`: the counts sum to 4096 and one of them is 512.
All inputs are finite; a program needn't handle non-finite values. No bound on the sum of `obs_count` on one device may be relied on, other than what follows from the above.
Results may differ from the reference program's by a relative error of at most 0.0003.
Values sent between devices are 32-bit elements; how exact they have to be, the bound alone decides.
A program may use at most 64 MiB of HBM per device.

```python
import math
import jax
import jax.numpy as jnp
import numpy as np
from jax import lax

MEM = 40
SLOTS = 7
LEV = 32
COL_DEV = 128
OBS_DEV = 512
COLS = 2048
OBS = 8192
CAP = 64
N_TILE = 16


def set_ends(result, own_key, low, largest):
    place = [jax.random.randint(jax.random.fold_in(own_key, axis), (), 0, length) for axis, length in enumerate(result.shape)]
    widest = result.shape.index(max(result.shape))
    neighbour = place[:widest] + [(place[widest] + 1) % result.shape[widest]] + place[widest + 1:]
    return result.at[tuple(place)].set(low).at[tuple(neighbour)].set(largest)


def level_of(key, shape, shards, low, largest):
    level = 1.0
    for axis_at, shards_of in shards:
        draws = jax.random.uniform(jax.random.fold_in(jax.random.fold_in(key, 6), axis_at), (shards_of,), jnp.float32, low / len(shards), largest / len(shards))
        level = level * jnp.repeat(jnp.exp(draws), shape[axis_at] // shards_of).reshape((-1,) + (1,) * (len(shape) - 1 - axis_at))
    return level


def split_up(number_of, total, limit, skew):
    portions = [(1 << 20) // math.isqrt(standing ** skew) + 1 for standing in range(2, number_of + 1)]
    spare, given = total - limit - (number_of - 1), [1] * (number_of - 1)
    while spare > 0:
        free = [i for i in range(number_of - 1) if given[i] < limit]
        mass, left = sum([portions[i] for i in free]), spare
        for i in free:
            extra = min(limit - given[i], max(1, left * portions[i] // mass), spare)
            given[i] = given[i] + extra
            spare = spare - extra
    return np.array([limit] + given)


def ragged(rng, count, total, limit, skew):
    if count == 2:
        one = jax.random.randint(rng, (), max(1, total - limit), min(limit, total - 1) + 1)
        return jnp.stack([one, total - one])
    lengths = jnp.asarray(split_up(count, total, limit, skew), jnp.int32)
    couples = (count - 1) // 2
    donor, taker = lengths[1:1 + 2 * couples:2], lengths[2:2 + 2 * couples:2]
    room = jnp.minimum(donor - 1, limit - taker)
    passed = jax.random.randint(jax.random.fold_in(rng, 1), (couples,), 0, 1 << 20) % (room + 1)
    lengths = lengths.at[1:1 + 2 * couples:2].set(donor - passed).at[2:2 + 2 * couples:2].set(taker + passed)
    return lengths[jax.random.permutation(jax.random.fold_in(rng, 2), count)]


def deal_out(rng, own, number, rows, number_of, top, limit, slope):
    order = jax.random.permutation(rng, number_of)
    crowded, common = load_shares(number_of, rows * top, limit, slope, True), load_shares(number_of, rows * top, limit, slope, False)
    places = jnp.arange(number_of)

    def named(sizes, turn):
        used = int((sizes > 0).sum())
        fixed = max(1, used // 4)
        shifted = fixed + (places - fixed + turn * (used - fixed)) % max(1, number_of - fixed)
        return jnp.zeros((number_of,), jnp.int32).at[order[jnp.where(places < fixed, places, shifted)]].set(jnp.asarray(sizes, jnp.int32))

    sizes = jnp.where(number % 4 == 0, named(crowded, number // 4), named(common, number - number // 4 - 1))
    mixed = jax.random.permutation(jax.random.fold_in(own, 3), number_of)
    giver, sink = mixed[0:number_of // 2 * 2:2], mixed[1:number_of // 2 * 2:2]
    slack = jnp.minimum(sizes[giver] - 1, limit - sizes[sink]) // 2
    slack = jnp.where((giver == order[0]) | (sink == order[0]) | (sizes[sink] == 0), 0, jnp.maximum(slack, 0))
    shifted = jax.random.randint(jax.random.fold_in(own, 4), (number_of // 2,), 0, 1 << 20) % (slack + 1)
    sizes = sizes.at[giver].add(-shifted).at[sink].add(shifted)
    items = jnp.searchsorted(jnp.cumsum(sizes), jnp.arange(rows * top), side="right").astype(jnp.int32)
    listing = items.reshape(top, rows).T
    listing = listing[jax.random.permutation(jax.random.fold_in(own, 1), rows)]
    turn = jax.random.randint(jax.random.fold_in(own, 2), (rows, 1), 0, top)
    return jnp.take_along_axis(listing, (jnp.arange(top)[None, :] + turn) % top, axis=1)


def load_shares(amount, total, most, slope, full):
    loads = [(1 << 20) // math.isqrt(standing ** slope) + 1 for standing in range(1, amount + 1)]
    largest = most if full else min(most, max(-(-total // amount), total * loads[0] // sum(loads)))
    least = 1 if total - largest >= amount - 1 else 0
    given, surplus = [largest] + [least] * (amount - 1), total - largest - least * (amount - 1)
    while surplus > 0:
        movable = [i for i in range(1, amount) if given[i] < largest] or [i for i in range(1, amount) if given[i] < most]
        pool, budget = sum([loads[i] for i in movable]), surplus
        for i in movable:
            more = min(most - given[i], max(1, budget * loads[i] // pool), surplus)
            given[i] = given[i] + more
            surplus = surplus - more
    return np.array(given)


def scatter_about(key, shape, scale, reach, pieces=(), held_as=jnp.bfloat16):
    level = level_of(key, shape, pieces, -0.22, 0.18) if pieces else 1.0
    entries = jax.random.normal(key, shape, jnp.float32) * scale * level
    return jnp.minimum(jnp.maximum(entries, -reach), reach).astype(held_as)


def setup_inputs(seed: int = 0) -> dict:
    key_of = jax.random.split(jax.random.key(seed), 9)
    ensemble = scatter_about(key_of[0], (MEM, SLOTS, LEV, COLS), 1.0, 6.0, ((0, 2), (3, 16)))
    control = scatter_about(key_of[1], (MEM, LEV, COLS), 1.0, 6.0, ((0, 2), (2, 16)))
    vert_loc = scatter_about(key_of[2], (LEV, LEV), LEV ** -0.5, 1.0)
    obs_source_keys = jax.random.split(jax.random.fold_in(key_of[3], 1), OBS // OBS_DEV)
    obs_source_turns = jax.random.permutation(jax.random.fold_in(key_of[3], 3), OBS // OBS_DEV)
    obs_source = jax.vmap(lambda own, number: deal_out(jax.random.fold_in(key_of[3], 2), own, number, OBS_DEV, N_TILE, 1, CAP, 2))(obs_source_keys, obs_source_turns).reshape((OBS, 1))
    obs_column = set_ends(jax.random.randint(key_of[4], (OBS,), 0, COL_DEV), jax.random.fold_in(key_of[4], 1), 0, COL_DEV - 1).astype(jnp.int32)
    obs_slot = set_ends(jax.random.randint(key_of[5], (OBS,), 0, SLOTS - 1), jax.random.fold_in(key_of[5], 1), 0, (SLOTS - 1) - 1).astype(jnp.int32)
    obs_frac = jnp.clip(1.0 * jax.random.uniform(key_of[6], (OBS,), jnp.float32) ** level_of(key_of[6], (OBS,), ((0, 16),), -0.2, 0.2), 0.0, 1.0)
    obs_count = ragged(key_of[7], N_TILE, OBS // 2, OBS_DEV, 2).astype(jnp.int32)
    return dict(ensemble=ensemble, control=control, vert_loc=vert_loc, obs_source=obs_source, obs_column=obs_column, obs_slot=obs_slot, obs_frac=obs_frac, obs_count=obs_count)


def reference(ensemble, control, vert_loc, obs_source, obs_column, obs_slot, obs_frac, obs_count):
    loc_float = vert_loc.astype(jnp.float32)

    def member_step(total, pair):
        member, ctrl = pair
        weighted = jnp.dot(loc_float, ctrl.astype(jnp.float32), precision=lax.Precision.HIGHEST)
        return total + member.astype(jnp.float32) * weighted[None], None

    start = jnp.zeros((SLOTS, LEV, COLS), jnp.float32)
    increment, _ = lax.scan(member_step, start, (ensemble, control))
    glob = (obs_source[:, 0] * COL_DEV + obs_column).astype(jnp.int32)
    lower = increment[obs_slot, :, glob].T
    upper = increment[obs_slot + 1, :, glob].T
    frac = obs_frac[None, :]
    value = (1.0 - frac) * lower + frac * upper
    live = (jnp.arange(OBS, dtype=jnp.int32) % OBS_DEV) < jnp.repeat(obs_count, OBS_DEV)
    return jnp.where(live[None, :], value, jnp.float32(0.0))
```

```python
import functools

import jax
import jax.numpy as jnp
from jax import lax
from jax.experimental import pallas as pl
from jax.experimental.pallas import tpu as pltpu
from jax.sharding import PartitionSpec as P

MESH = pl.DeviceIdType.MESH
LANES = 128
F32 = jnp.float32
BF16 = jnp.bfloat16


def iota(shape, axis):
    return lax.broadcasted_iota(jnp.int32, shape, axis)


def one_hot(condition):
    return jnp.where(condition, F32(1.0), F32(0.0)).astype(BF16)


def dot(a, b):
    return jnp.dot(a, b, preferred_element_type=F32)


def dot_nt(a, b):
    return lax.dot_general(a, b, (((1,), (1,)), ((), ())), preferred_element_type=F32)


def two_pieces(x):
    high = x.astype(BF16)
    return high, (x - high.astype(F32)).astype(BF16)


def turned(x, shift):
    shift = shift % LANES
    return x if shift == 0 else pltpu.roll(x, shift, 1)


def kernel(
    tiles, groups, cap, packs,
    ens_hbm, ctl_hbm, vloc_ref, source_ref, column_ref, slot_ref, frac_ref, count_ref,
    out_ref,
    ens, ctl, weighted, part, part_in, req_out, req_in, res_out, res_in, place,
    load_sem, part_send, part_recv, req_send, req_recv, res_send, res_recv,
):
    me = lax.axis_index("tile")
    mine = lax.axis_index("member")
    members, slots, levels, cols = ens.shape
    share = levels // groups
    rows = share // packs
    obs = column_ref.shape[1]
    owners = LANES // cap
    spans = tiles * cap // LANES

    def peer(step):
        return lax.rem(me + step, tiles)

    def partner(step):
        return lax.rem(mine + step, groups)

    load_ctl = pltpu.make_async_copy(ctl_hbm, ctl, load_sem.at[0])
    load_ens = pltpu.make_async_copy(ens_hbm, ens, load_sem.at[1])
    load_ctl.start()
    load_ens.start()

    barrier = pltpu.get_barrier_semaphore()

    def greet(index, carry):
        step, side = index // groups, lax.rem(index, groups)
        pl.semaphore_signal(
            barrier, inc=1, device_id={"tile": peer(step), "member": partner(side)},
            device_id_type=MESH,
        )
        return carry

    lax.fori_loop(1, tiles * groups, greet, 0)

    source = source_ref[...]
    hits = source == iota((tiles, obs), 0)
    hits_f = jnp.where(hits, F32(1.0), F32(0.0))
    before = one_hot(iota((LANES, LANES), 0) < iota((LANES, LANES), 1))
    seen = jnp.zeros((tiles, 1), F32)
    ranks = []
    for block in range(obs // LANES):
        hit = hits_f[:, block * LANES:(block + 1) * LANES]
        ahead = dot(hit.astype(BF16), before) + seen
        ranks.append(jnp.sum(ahead * hit, axis=0, keepdims=True))
        seen = seen + jnp.sum(hit, axis=1, keepdims=True)
    rank = jnp.concatenate(ranks, axis=1).astype(jnp.int32)
    spread = one_hot(rank == lax.rem(iota((LANES, obs), 0), cap))
    frac = frac_ref[...]
    frac_0 = frac.astype(BF16).astype(F32)
    frac_1 = (frac - frac_0).astype(BF16).astype(F32)
    frac_2 = frac - frac_0 - frac_1
    values = [column_ref[...].astype(F32), slot_ref[...].astype(F32), frac_0, frac_1, frac_2]
    packed = dot_nt(
        jnp.concatenate([jnp.where(hits, v, F32(0.0)) for v in values], axis=0).astype(BF16), spread
    )
    packed = [packed[i * tiles:(i + 1) * tiles] for i in range(len(values))]
    request = jnp.where(
        iota((tiles, LANES), 1) < cap,
        packed[0] + cols * packed[1],
        packed[2] + packed[3] + packed[4],
    )
    for tile in range(tiles):
        req_out[tile] = request[tile:tile + 1]

    pl.semaphore_wait(barrier, tiles * groups - 1)

    def ask(step):
        return pltpu.make_async_remote_copy(
            src_ref=req_out.at[peer(step)], dst_ref=req_in.at[me],
            send_sem=req_send.at[peer(step)], recv_sem=req_recv.at[me],
            device_id={"tile": peer(step), "member": mine}, device_id_type=MESH,
        )

    def asked(step):
        return pltpu.make_async_remote_copy(
            src_ref=req_out.at[peer(step)], dst_ref=req_in.at[peer(step)],
            send_sem=req_send.at[peer(step)], recv_sem=req_recv.at[peer(step)],
            device_id={"tile": peer(step), "member": mine}, device_id_type=MESH,
        )

    def send_request(step, carry):
        ask(step).start()
        return carry

    lax.fori_loop(1, tiles, send_request, 0)
    req_in[me] = req_out[me]

    batch = max(d for d in range(1, max(1, LANES // levels) + 1) if members % d == 0)
    wide = batch * levels
    repeat = one_hot(lax.rem(iota((wide, levels), 0), levels) == iota((wide, levels), 1))
    tall = dot(repeat, vloc_ref[...]).astype(BF16)
    full = dot_nt(tall, repeat)
    factor = jnp.where(
        iota((wide, wide), 0) // levels == iota((wide, wide), 1) // levels, full, F32(0.0)
    ).astype(BF16)
    load_ctl.wait()
    for step in range(members // batch):
        weighted[step * wide:(step + 1) * wide] = dot(factor, ctl[step * wide:(step + 1) * wide])

    load_ens.wait()
    for slot in range(slots):
        total = jnp.zeros((levels, cols), F32)
        for k in range(members):
            total = total + ens[k, slot].astype(F32) * weighted[k * levels:(k + 1) * levels]
        for group in range(groups):
            part[group, slot] = total[group * share:(group + 1) * share]

    def give(step):
        return pltpu.make_async_remote_copy(
            src_ref=part.at[partner(step)], dst_ref=part_in.at[step - 1],
            send_sem=part_send.at[step - 1], recv_sem=part_recv.at[step - 1],
            device_id={"tile": me, "member": partner(step)}, device_id_type=MESH,
        )

    for step in range(1, groups):
        give(step).start()

    position = source * cap + rank
    place[...] = one_hot(position == iota((tiles * cap, obs), 0))

    for step in range(1, groups):
        give(step).wait_recv()
    increment = part[mine]
    for step in range(1, groups):
        increment = increment + part_in[step - 1]
    pieces = jnp.concatenate(two_pieces(increment.reshape(slots * share, cols)), axis=1)

    def wait_request(step, carry):
        asked(step).wait_recv()
        return carry

    lax.fori_loop(1, tiles, wait_request, 0)

    lane = iota((1, LANES), 1)
    codes, fracs = [], []
    for span in range(spans):
        code = jnp.zeros((1, LANES), F32)
        part_of = jnp.zeros((1, LANES), F32)
        for i in range(owners):
            got = req_in[span * owners + i]
            here = lane // cap == i
            code = jnp.where(here, turned(got, i * cap), code)
            part_of = jnp.where(here, turned(got, i * cap - cap), part_of)
        codes.append(code)
        fracs.append(part_of)
    code = jnp.concatenate(codes, axis=1).astype(jnp.int32)
    frac = jnp.concatenate(fracs, axis=1)
    wanted = code // cols
    column = code - wanted * cols
    width = tiles * cap
    picked = one_hot(lax.rem(iota((2 * cols, width), 0), cols) == column)
    columns = dot(pieces, picked)
    answer = jnp.zeros((share, width), F32)
    for slot in range(slots):
        weight = jnp.where(wanted == slot, 1.0 - frac, jnp.where(wanted + 1 == slot, frac, F32(0.0)))
        answer = answer + weight * columns[slot * share:(slot + 1) * share]
    for owner in range(tiles):
        first = owner * cap // LANES * LANES
        offset = owner * cap % LANES
        packet = jnp.zeros((rows, LANES), F32)
        for j in range(packs):
            block = answer[j * rows:(j + 1) * rows, first:first + LANES]
            packet = jnp.where(lane // cap == j, turned(block, j * cap - offset), packet)
        res_out[owner] = packet

    def reply(index):
        step, side = index // groups, lax.rem(index, groups)
        return pltpu.make_async_remote_copy(
            src_ref=res_out.at[peer(step)], dst_ref=res_in.at[mine, me],
            send_sem=res_send.at[partner(side), peer(step)], recv_sem=res_recv.at[mine, me],
            device_id={"tile": peer(step), "member": partner(side)}, device_id_type=MESH,
        )

    def replied(index):
        step, side = index // groups, lax.rem(index, groups)
        return pltpu.make_async_remote_copy(
            src_ref=res_out.at[peer(step)], dst_ref=res_in.at[partner(side), peer(step)],
            send_sem=res_send.at[partner(side), peer(step)],
            recv_sem=res_recv.at[partner(side), peer(step)],
            device_id={"tile": peer(step), "member": partner(side)}, device_id_type=MESH,
        )

    def send_reply(index, carry):
        reply(index).start()
        return carry

    def wait_reply(index, carry):
        replied(index).wait_recv()
        return carry

    lax.fori_loop(1, tiles * groups, send_reply, 0)
    res_in[mine, me] = res_out[me]
    lax.fori_loop(1, tiles * groups, wait_reply, 0)

    bands = []
    for group in range(groups):
        for j in range(packs):
            band = []
            for span in range(spans):
                tile = jnp.zeros((rows, LANES), F32)
                for i in range(owners):
                    got = res_in[group, span * owners + i]
                    tile = jnp.where(lane // cap == i, turned(got, i * cap - j * cap), tile)
                band.append(tile)
            bands.append(jnp.concatenate(band, axis=1))
    high, low = two_pieces(jnp.concatenate(bands, axis=0))
    both = dot(jnp.concatenate([high, low], axis=0), place[...])
    value = both[:levels] + both[levels:]
    live = iota((levels, obs), 1) < count_ref[0]
    out_ref[...] = jnp.where(live, value, F32(0.0))

    for step in range(1, groups):
        give(step).wait_send()

    def wait_sends(step, carry):
        ask(step).wait_send()
        return carry

    def wait_reply_sends(index, carry):
        reply(index).wait_send()
        return carry

    lax.fori_loop(1, tiles, wait_sends, 0)
    lax.fori_loop(1, tiles * groups, wait_reply_sends, 0)


def on_device(ensemble, control, vert_loc, obs_source, obs_column, obs_slot, obs_frac, obs_count):
    tiles, groups = lax.axis_size("tile"), lax.axis_size("member")
    members, slots, levels, cols = ensemble.shape
    obs = obs_column.shape[0]
    cap = max(4, 2 * obs // tiles)
    share = levels // groups
    packs = max(1, min(LANES // cap, share // 8))
    rows = share // packs
    vmem = pl.BlockSpec(memory_space=pltpu.VMEM)
    hbm = pl.BlockSpec(memory_space=pl.ANY)
    smem = pl.BlockSpec(memory_space=pltpu.SMEM)
    dma = pltpu.SemaphoreType.DMA
    return pl.pallas_call(
        functools.partial(kernel, tiles, groups, cap, packs),
        out_shape=jax.ShapeDtypeStruct((levels, obs), F32),
        in_specs=[hbm, hbm, vmem, vmem, vmem, vmem, vmem, smem],
        out_specs=vmem,
        scratch_shapes=[
            pltpu.VMEM((members, slots, levels, cols), BF16),
            pltpu.VMEM((members * levels, cols), BF16),
            pltpu.VMEM((members * levels, cols), F32),
            pltpu.VMEM((groups, slots, share, cols), F32),
            pltpu.VMEM((max(1, groups - 1), slots, share, cols), F32),
            pltpu.VMEM((tiles, 1, LANES), F32),
            pltpu.VMEM((tiles, 1, LANES), F32),
            pltpu.VMEM((tiles, rows, LANES), F32),
            pltpu.VMEM((groups, tiles, rows, LANES), F32),
            pltpu.VMEM((tiles * cap, obs), BF16),
            dma((2,)),
            dma((max(1, groups - 1),)),
            dma((max(1, groups - 1),)),
            dma((tiles,)),
            dma((tiles,)),
            dma((groups, tiles)),
            dma((groups, tiles)),
        ],
        compiler_params=pltpu.CompilerParams(collective_id=0, has_side_effects=True),
    )(
        ensemble,
        control.reshape(members * levels, cols),
        vert_loc,
        obs_source.reshape(1, obs),
        obs_column.reshape(1, obs),
        obs_slot.reshape(1, obs),
        obs_frac.reshape(1, obs),
        obs_count,
    )


def solution(mesh):
    placed = (
        P("member", None, None, "tile"),
        P("member", None, "tile"),
        P(),
        P("tile", None),
        P("tile"),
        P("tile"),
        P("tile"),
        P("tile"),
    )
    return jax.shard_map(
        on_device, mesh=mesh, in_specs=placed, out_specs=P(None, "tile"), check_vma=False
    )
```

```python
import functools

import jax
import jax.numpy as jnp
from jax import lax
from jax.experimental import pallas as pl
from jax.experimental.pallas import tpu as pltpu
from jax.sharding import PartitionSpec as P

MESH = pl.DeviceIdType.MESH
LANES = 128
F32 = jnp.float32
BF16 = jnp.bfloat16


def iota(shape, axis):
    return lax.broadcasted_iota(jnp.int32, shape, axis)


def one_hot(condition):
    return jnp.where(condition, F32(1.0), F32(0.0)).astype(BF16)


def dot(a, b):
    return jnp.dot(a, b, preferred_element_type=F32)


def dot_nt(a, b):
    return lax.dot_general(a, b, (((1,), (1,)), ((), ())), preferred_element_type=F32)


def two_pieces(x):
    high = x.astype(BF16)
    return high, (x - high.astype(F32)).astype(BF16)


def turned(x, shift):
    shift = shift % LANES
    return x if shift == 0 else pltpu.roll(x, shift, 1)


def kernel(
    tiles, groups, cap, packs,
    ens_hbm, ctl_hbm, vloc_hbm, source_hbm, column_hbm, slot_hbm, frac_hbm, count_ref,
    out_ref,
    vloc_ref, source_ref, column_ref, slot_ref, frac_ref, ens, ctl, weighted, part, part_in, req_out, req_in, res_out, res_in, place,
    load_sem, part_send, part_recv, req_send, req_recv, res_send, res_recv,
):
    me = lax.axis_index("tile")
    mine = lax.axis_index("member")
    members, slots, levels, cols = ens.shape
    share = levels // groups
    rows = share // packs
    obs = column_ref.shape[1]
    owners = LANES // cap
    spans = tiles * cap // LANES

    def loaded(index, source, target):
        return pltpu.make_async_copy(source, target, load_sem.at[index])

    loads = [
        loaded(0, source_hbm, source_ref), loaded(1, column_hbm, column_ref),
        loaded(2, slot_hbm, slot_ref), loaded(3, frac_hbm, frac_ref),
        loaded(4, vloc_hbm, vloc_ref), loaded(5, ctl_hbm, ctl), loaded(6, ens_hbm, ens),
    ]
    for load in loads[:4]:
        load.start()

    stride = jnp.where(2 * me < tiles, 1, tiles - 1)
    span_stride = jnp.where(2 * me < tiles, 1, spans - 1)
    home = me // owners

    def peer(step):
        return lax.rem(me + stride * step, tiles)

    def span_at(step):
        return lax.rem(home + span_stride * step, spans)

    def partner(step):
        return lax.rem(mine + step, groups)

    def far_first(count, body):
        if count <= 64:
            for index in range(count - 1, 0, -1):
                body(index)
        else:
            lax.fori_loop(1, count, lambda index, carry: (body(index), carry)[1], 0)

    barrier = pltpu.get_barrier_semaphore()

    def greet(index):
        step, side = index // groups, index % groups
        pl.semaphore_signal(
            barrier, inc=1, device_id={"tile": peer(step), "member": partner(side)},
            device_id_type=MESH,
        )

    far_first(tiles * groups, greet)
    for load in loads[4:]:
        load.start()

    for load in loads[:4]:
        load.wait()
    source = source_ref[...]
    hits = source == iota((tiles, obs), 0)
    hits_f = jnp.where(hits, F32(1.0), F32(0.0))
    before = one_hot(iota((LANES, LANES), 0) < iota((LANES, LANES), 1))
    seen = jnp.zeros((tiles, 1), F32)
    ranks = []
    for block in range(obs // LANES):
        hit = hits_f[:, block * LANES:(block + 1) * LANES]
        ahead = dot(hit.astype(BF16), before) + seen
        ranks.append(jnp.sum(ahead * hit, axis=0, keepdims=True))
        seen = seen + jnp.sum(hit, axis=1, keepdims=True)
    rank = jnp.concatenate(ranks, axis=1).astype(jnp.int32)
    spread = one_hot(rank == lax.rem(iota((LANES, obs), 0), cap))
    frac = frac_ref[...]
    frac_0 = frac.astype(BF16).astype(F32)
    frac_1 = (frac - frac_0).astype(BF16).astype(F32)
    frac_2 = frac - frac_0 - frac_1
    values = [column_ref[...].astype(F32), slot_ref[...].astype(F32), frac_0, frac_1, frac_2]
    packed = dot_nt(
        jnp.concatenate([jnp.where(hits, v, F32(0.0)) for v in values], axis=0).astype(BF16), spread
    )
    packed = [packed[i * tiles:(i + 1) * tiles] for i in range(len(values))]
    request = jnp.where(
        iota((tiles, LANES), 1) < cap,
        packed[0] + cols * packed[1],
        packed[2] + packed[3] + packed[4],
    )
    for tile in range(tiles):
        req_out[tile] = request[tile:tile + 1]

    pl.semaphore_wait(barrier, tiles * groups - 1)

    def request_to(tile, slot_of):
        return pltpu.make_async_remote_copy(
            src_ref=req_out.at[tile], dst_ref=req_in.at[slot_of],
            send_sem=req_send.at[tile], recv_sem=req_recv.at[slot_of],
            device_id={"tile": tile, "member": mine}, device_id_type=MESH,
        )

    far_first(tiles, lambda step: request_to(peer(step), me).start())
    req_in[me] = req_out[me]

    batch = max(d for d in range(1, max(1, LANES // levels) + 1) if members % d == 0)
    wide = batch * levels
    repeat = one_hot(lax.rem(iota((wide, levels), 0), levels) == iota((wide, levels), 1))
    for load in loads[4:6]:
        load.wait()
    tall = dot(repeat, vloc_ref[...]).astype(BF16)
    full = dot_nt(tall, repeat)
    factor = jnp.where(
        iota((wide, wide), 0) // levels == iota((wide, wide), 1) // levels, full, F32(0.0)
    ).astype(BF16)
    for step in range(members // batch):
        weighted[step * wide:(step + 1) * wide] = dot(factor, ctl[step * wide:(step + 1) * wide])

    loads[6].wait()
    for slot in range(slots):
        total = jnp.zeros((levels, cols), F32)
        for k in range(members):
            total = total + ens[k, slot].astype(F32) * weighted[k * levels:(k + 1) * levels]
        for group in range(groups):
            part[group, slot] = total[group * share:(group + 1) * share]

    def give(step):
        return pltpu.make_async_remote_copy(
            src_ref=part.at[partner(step)], dst_ref=part_in.at[step - 1],
            send_sem=part_send.at[step - 1], recv_sem=part_recv.at[step - 1],
            device_id={"tile": me, "member": partner(step)}, device_id_type=MESH,
        )

    for step in range(1, groups):
        give(step).start()

    position = source * cap + rank
    place[...] = one_hot(position == iota((tiles * cap, obs), 0))

    for step in range(1, groups):
        give(step).wait_recv()
    increment = part[mine]
    for step in range(1, groups):
        increment = increment + part_in[step - 1]
    pieces = jnp.concatenate(two_pieces(increment.reshape(slots * share, cols)), axis=1)

    def reply_to(tile, side, slot_of, from_group):
        return pltpu.make_async_remote_copy(
            src_ref=res_out.at[tile], dst_ref=res_in.at[from_group, slot_of],
            send_sem=res_send.at[partner(side), tile], recv_sem=res_recv.at[from_group, slot_of],
            device_id={"tile": tile, "member": partner(side)}, device_id_type=MESH,
        )

    def unless_me(step, tile, body):
        if step == 0:
            pl.when(tile != me)(body)
        else:
            body()

    lane = iota((1, LANES), 1)
    for step in range(spans):
        span = span_at(step)
        code = jnp.zeros((1, LANES), F32)
        frac = jnp.zeros((1, LANES), F32)
        for i in range(owners):
            tile = span * owners + i
            unless_me(step, tile, lambda tile=tile: request_to(tile, tile).wait_recv())
            got = req_in[tile]
            here = lane // cap == i
            code = jnp.where(here, turned(got, i * cap), code)
            frac = jnp.where(here, turned(got, i * cap - cap), frac)
        code = code.astype(jnp.int32)
        wanted = code // cols
        column = code - wanted * cols
        columns = dot(pieces, one_hot(lax.rem(iota((2 * cols, LANES), 0), cols) == column))
        answer = jnp.zeros((share, LANES), F32)
        for slot in range(slots):
            weight = jnp.where(
                wanted == slot, 1.0 - frac, jnp.where(wanted + 1 == slot, frac, F32(0.0))
            )
            answer = answer + weight * columns[slot * share:(slot + 1) * share]
        for i in range(owners):
            tile = span * owners + i
            packet = jnp.zeros((rows, LANES), F32)
            for j in range(packs):
                block = answer[j * rows:(j + 1) * rows]
                packet = jnp.where(lane // cap == j, turned(block, (j - i) * cap), packet)
            res_out[tile] = packet
            if step == 0:
                @pl.when(tile == me)
                def _():
                    res_in[mine, me] = packet
            for side in range(groups):
                if side == 0:
                    unless_me(step, tile, lambda tile=tile: reply_to(tile, 0, me, mine).start())
                else:
                    reply_to(tile, side, me, mine).start()

    for step in range(1, groups):
        give(step).wait_send()

    def wait_reply_send(index):
        reply_to(peer(index // groups), index % groups, me, mine).wait_send()

    far_first(tiles, lambda step: request_to(peer(step), me).wait_send())
    far_first(tiles * groups, wait_reply_send)

    live = iota((levels, obs), 1) < count_ref[0]
    both = jnp.zeros((2 * levels, obs), F32)
    for step in range(spans):
        span = span_at(step)
        bands = [jnp.zeros((rows, LANES), F32)] * (groups * packs)
        for side in range(groups):
            for i in range(owners):
                tile = span * owners + i
                body = lambda tile=tile, side=side: reply_to(tile, side, tile, partner(side)).wait_recv()
                if side == 0:
                    unless_me(step, tile, body)
                else:
                    body()
        for group in range(groups):
            for i in range(owners):
                got = res_in[group, span * owners + i]
                for j in range(packs):
                    at = group * packs + j
                    bands[at] = jnp.where(lane // cap == i, turned(got, (i - j) * cap), bands[at])
        high, low = two_pieces(jnp.concatenate(bands, axis=0))
        first = pl.multiple_of(span * LANES, LANES)
        both = both + dot(jnp.concatenate([high, low], axis=0), place[pl.ds(first, LANES)])
    out_ref[...] = jnp.where(live, both[:levels] + both[levels:], F32(0.0))


def on_device(ensemble, control, vert_loc, obs_source, obs_column, obs_slot, obs_frac, obs_count):
    tiles, groups = lax.axis_size("tile"), lax.axis_size("member")
    members, slots, levels, cols = ensemble.shape
    obs = obs_column.shape[0]
    cap = max(4, 2 * obs // tiles)
    share = levels // groups
    packs = max(1, min(LANES // cap, share // 8))
    rows = share // packs
    vmem = pl.BlockSpec(memory_space=pltpu.VMEM)
    hbm = pl.BlockSpec(memory_space=pl.ANY)
    dma = pltpu.SemaphoreType.DMA
    return pl.pallas_call(
        functools.partial(kernel, tiles, groups, cap, packs),
        out_shape=pltpu.VMEM((levels, obs), F32),
        in_specs=[hbm] * 7 + [pl.BlockSpec(memory_space=pltpu.SMEM)],
        out_specs=vmem,
        scratch_shapes=[
            pltpu.VMEM((levels, levels), BF16),
            pltpu.VMEM((1, obs), jnp.int32),
            pltpu.VMEM((1, obs), jnp.int32),
            pltpu.VMEM((1, obs), jnp.int32),
            pltpu.VMEM((1, obs), F32),
            pltpu.VMEM((members, slots, levels, cols), BF16),
            pltpu.VMEM((members * levels, cols), BF16),
            pltpu.VMEM((members * levels, cols), F32),
            pltpu.VMEM((groups, slots, share, cols), F32),
            pltpu.VMEM((max(1, groups - 1), slots, share, cols), F32),
            pltpu.VMEM((tiles, 1, LANES), F32),
            pltpu.VMEM((tiles, 1, LANES), F32),
            pltpu.VMEM((tiles, rows, LANES), F32),
            pltpu.VMEM((groups, tiles, rows, LANES), F32),
            pltpu.VMEM((tiles * cap, obs), BF16),
            dma((7,)),
            dma((max(1, groups - 1),)),
            dma((max(1, groups - 1),)),
            dma((tiles,)),
            dma((tiles,)),
            dma((groups, tiles)),
            dma((groups, tiles)),
        ],
        compiler_params=pltpu.CompilerParams(collective_id=0, has_side_effects=True),
    )(
        ensemble,
        control.reshape(members * levels, cols),
        vert_loc,
        obs_source.reshape(1, obs),
        obs_column.reshape(1, obs),
        obs_slot.reshape(1, obs),
        obs_frac.reshape(1, obs),
        obs_count,
    )


def solution(mesh):
    placed = (
        P("member", None, None, "tile"),
        P("member", None, "tile"),
        P(),
        P("tile", None),
        P("tile"),
        P("tile"),
        P("tile"),
        P("tile"),
    )
    return jax.shard_map(
        on_device, mesh=mesh, in_specs=placed, out_specs=P(None, "tile"), check_vma=False
    )
```
